128 devices in a mesh: dp: 1, sp: 128 (over z, y, x, core).
Axes of the slice: x: 4, y: 4, z: 4, core: 2. Of those that a mesh axis runs over, the one named last changes fastest.
Arguments:
- tokens: bfloat16 [128, 2048], P('dp')
- w_query: bfloat16 [2048, 2048], replicated
- w_key: bfloat16 [2048, 256], replicated
- w_value: bfloat16 [2048, 256], replicated
- w_out: bfloat16 [2048, 2048], P('sp')
- k_cache: bfloat16 [128, 4096, 256], P('dp', 'sp')
- v_cache: bfloat16 [128, 4096, 256], P('dp', 'sp')
- positions: int32 [128], P('dp')
Outputs:
- output 1: bfloat16 [128, 2048], P('dp')
- output 2: bfloat16 [128, 4096, 256], P('dp', 'sp')
- output 3: bfloat16 [128, 4096, 256], P('dp', 'sp')
All inputs are finite; a program needn't handle non-finite values.
Results may differ from the reference program's by a relative error of at most 0.00402255.
Values are sent between devices in bfloat16 or wider.
A program may use at most 1 GiB of HBM per device.

```python
import jax
import jax.numpy as jnp
import math
from jax import lax

BATCH_ROWS = 128
SEQ_LEN = 4096
D_MODEL = 2048
N_HEADS = 8
HEAD_DIM = 256
GAIN_BLOCK = 32


def setup_inputs(seed: int = 0, part: int = 0) -> dict:
    root = jax.random.key(seed)
    shared = jax.random.split(root, 4)
    local = jax.random.split(jax.random.fold_in(root, part), 5)
    q_width = N_HEADS * HEAD_DIM
    align_scale = (math.log(SEQ_LEN) + 0.5) * HEAD_DIM ** -0.5
    tokens = jax.random.normal(local[0], (BATCH_ROWS, D_MODEL), jnp.float32)
    key_raw = jax.random.normal(shared[1], (D_MODEL, HEAD_DIM), jnp.float32)
    w_query = (jax.random.normal(shared[0], (D_MODEL, q_width), jnp.float32) + align_scale * jnp.tile(key_raw, (1, N_HEADS))) * D_MODEL ** -0.5
    w_key = key_raw * D_MODEL ** -0.5
    w_value = jax.random.normal(shared[2], (D_MODEL, HEAD_DIM), jnp.float32) * D_MODEL ** -0.5
    w_out = jax.random.normal(shared[3], (q_width, D_MODEL), jnp.float32) * q_width ** -0.5
    n_blocks = SEQ_LEN // GAIN_BLOCK
    key_gains = jax.random.uniform(local[1], (BATCH_ROWS, n_blocks, 1, 1), jnp.float32, 0.6, 1.6)
    k_cache = (jax.random.normal(local[2], (BATCH_ROWS, n_blocks, GAIN_BLOCK, HEAD_DIM), jnp.float32) * key_gains).reshape(BATCH_ROWS, SEQ_LEN, HEAD_DIM)
    v_cache = jax.random.normal(local[3], (BATCH_ROWS, SEQ_LEN, HEAD_DIM), jnp.float32)
    positions = jax.random.randint(local[4], (BATCH_ROWS,), SEQ_LEN // 4, SEQ_LEN, jnp.int32)
    positions = positions.at[0].set(SEQ_LEN - 1).at[1].set(SEQ_LEN // 4)
    return dict(tokens=tokens.astype(jnp.bfloat16), w_query=w_query.astype(jnp.bfloat16), w_key=w_key.astype(jnp.bfloat16), w_value=w_value.astype(jnp.bfloat16), w_out=w_out.astype(jnp.bfloat16), k_cache=k_cache.astype(jnp.bfloat16), v_cache=v_cache.astype(jnp.bfloat16), positions=positions)


def reference(tokens, w_query, w_key, w_value, w_out, k_cache, v_cache, positions):
    queries = jnp.dot(tokens, w_query, preferred_element_type=jnp.float32).astype(jnp.bfloat16)
    queries = queries.reshape(BATCH_ROWS, N_HEADS, HEAD_DIM)
    key_new = jnp.dot(tokens, w_key, preferred_element_type=jnp.float32).astype(jnp.bfloat16)
    value_new = jnp.dot(tokens, w_value, preferred_element_type=jnp.float32).astype(jnp.bfloat16)
    slot_ids = jnp.arange(SEQ_LEN)
    hit_mask = (slot_ids[None, :] == positions[:, None])[:, :, None]
    k_upd = jnp.where(hit_mask, key_new[:, None, :], k_cache)
    v_upd = jnp.where(hit_mask, value_new[:, None, :], v_cache)

    def one_row(row_args):
        q_row, k_row, v_row, pos_row = row_args
        scores = jnp.dot(q_row, k_row.T, preferred_element_type=jnp.float32) * HEAD_DIM ** -0.5
        scores = jnp.where(slot_ids[None, :] <= pos_row, scores, -jnp.inf)
        weights = jnp.exp(scores - jnp.max(scores, axis=1, keepdims=True))
        weight_sum = jnp.sum(weights, axis=1)
        value_sum = jnp.dot(weights.astype(jnp.bfloat16), v_row, preferred_element_type=jnp.float32)
        return value_sum / weight_sum[:, None]

    head_outs = lax.map(one_row, (queries, k_upd, v_upd, positions))
    attn_heads = head_outs.astype(jnp.bfloat16).reshape(BATCH_ROWS, N_HEADS * HEAD_DIM)
    attn_out = jnp.dot(attn_heads, w_out, preferred_element_type=jnp.float32).astype(jnp.bfloat16)
    return (attn_out, k_upd, v_upd)
```

```python
import jax
import jax.numpy as jnp
from jax import lax
from jax.experimental import pallas as pl
from jax.experimental.pallas import tpu as pltpu
from jax.sharding import PartitionSpec as P

F32 = jnp.float32
BF16 = jnp.bfloat16
SIDE = 4
MESH = pl.DeviceIdType.MESH
LOWEST = float(jnp.finfo(jnp.float32).min)


def attention_kernel(pos_ref, q_ref, k_ref, v_ref, wo_ref, out_ref,
                     qs, own, r0, s1, r1, s2, r2, s3, r3, osc, w1, wo_all, y_all,
                     d0_s, d0_r, wz_s, wz_r, wg_s, wg_r, s1_s, s1_r, s2_s, s2_r, s3_s, s3_r,
                     o_s, o_r, yz_s, yz_r, yg_s, yg_r, yd_s, yd_r):
    me = lax.axis_index('sp')
    c = lax.rem(me, 2)
    x = lax.rem(me // 2, SIDE)
    y = lax.rem(me // 8, SIDE)
    z = me // 32
    base = me * 32

    def dev(zz, yy, xx, cc):
        return {'sp': ((zz * SIDE + yy) * SIDE + xx) * 2 + cc}

    def fwd(a, d):
        return lax.rem(a + d, SIDE)

    mate = dev(z, y, x, 1 - c)
    x_peer = [None] + [dev(z, y, fwd(x, d), c) for d in (1, 2, 3)]
    y_peer = [None] + [dev(z, fwd(y, d), x, c) for d in (1, 2, 3)]
    z_peer = [None] + [dev(fwd(z, d), y, x, c) for d in (1, 2, 3)]

    barrier = pltpu.get_barrier_semaphore()
    for peer in [mate] + x_peer[1:] + y_peer[1:] + z_peer[1:]:
        pl.semaphore_signal(barrier, inc=1, device_id=peer, device_id_type=MESH)

    def rcopy(src, dst, ssem, rsem, peer):
        return pltpu.make_async_remote_copy(src_ref=src, dst_ref=dst, send_sem=ssem, recv_sem=rsem,
                                            device_id=peer, device_id_type=MESH)

    for h in range(8):
        qh = q_ref[:, h * 256:(h + 1) * 256].astype(F32).reshape(16, 8, 256)
        qs[:, h] = qh

    pl.semaphore_wait(barrier, 10)

    pend = []
    w_mate = rcopy(wo_ref.at[:, pl.ds(pl.multiple_of((1 - c) * 1024, 1024), 1024)], w1, wz_s.at[6], wz_r.at[6], mate)
    w_mate.start()
    wz = []
    for d in (1, 2, 3):
        zz = fwd(z, d)
        cp = rcopy(wo_ref.at[:, pl.ds(pl.multiple_of(c * 1024 + zz * 256, 256), 256)], wo_all.at[z, y, x, c],
                   wz_s.at[d - 1], wz_r.at[d - 1], z_peer[d])
        cp.start()
        wz.append(cp)
    wo_all[z, y, x, c] = wo_ref[:, pl.ds(pl.multiple_of(c * 1024 + z * 256, 256), 256)]

    lane = lax.broadcasted_iota(jnp.int32, (8, 128), 1)
    sub256 = lax.broadcasted_iota(jnp.int32, (8, 256), 0)
    col_t = lax.broadcasted_iota(jnp.int32, (8, 256), 1) - 32 * sub256

    def tile_of(r):
        gy = fwd(y, 1 + r // SIDE)
        gx = fwd(x, 1 + lax.rem(r, SIDE))
        return gy, gx

    def d0_copy(r, g):
        return rcopy(own.at[g, 1 - c], r0.at[g], d0_s.at[r], d0_r.at[r], mate)

    def attend(r):
        gy, gx = tile_of(r)
        g = gy * SIDE + gx
        kg = k_ref[pl.ds(g * 8, 8)].reshape(256, 256)
        vg = v_ref[pl.ds(g * 8, 8)].reshape(256, 256)
        qg = qs[g].reshape(64, 256).astype(BF16)
        s = lax.dot_general(qg, kg, (((1,), (1,)), ((), ())), preferred_element_type=F32) * 0.0625
        lim = jnp.zeros((8, 256), jnp.int32)
        for j in range(8):
            lim = jnp.where(sub256 == j, pos_ref[g * 8 + j] - base, lim)
        valid = (col_t >= 0) & (col_t < 32) & (col_t <= lim)
        s = jnp.where(valid[None], s.reshape(8, 8, 256), -jnp.inf)
        m = jnp.maximum(jnp.max(s, axis=2, keepdims=True), LOWEST)
        w = jnp.exp(s - m)
        l = jnp.sum(w, axis=2, keepdims=True)
        o = jnp.dot(w.astype(BF16).reshape(64, 256), vg, preferred_element_type=F32).reshape(8, 8, 256)
        for half in range(2):
            for st in range(2):
                h0 = half * 4 + st * 2
                for j in range(2):
                    for k in range(2):
                        own[g, half, st, 2 * j + k] = o[h0 + j, :, k * 128:(k + 1) * 128]
                own[g, half, st, 4] = jnp.where(lane == 0, m[h0], jnp.where(lane == 1, m[h0 + 1], jnp.where(
                    lane == 2, l[h0], l[h0 + 1])))
        d0_copy(r, g).start()

    def combine(parts):
        stats = [p[4] for p in parts]
        top = stats[0]
        for t in stats[1:]:
            top = jnp.maximum(top, t)
        data = [None] * 4
        total = None
        for p, t in zip(parts, stats):
            a = jnp.exp(t - top)
            f = [jnp.broadcast_to(a[:, j:j + 1], (8, 128)) for j in range(2)]
            for i in range(4):
                term = p[i] * f[i // 2]
                data[i] = term if data[i] is None else data[i] + term
            term = t * jnp.where(lane % 2 == 0, f[0], f[1])
            total = term if total is None else total + term
        return data, top, total

    def put(dst, parts):
        data, top, total = combine(parts)
        for i in range(4):
            dst[i] = data[i]
        dst[4] = jnp.where(lane < 2, top, total)

    def s1_copy(st, d, g, idx, peer):
        return rcopy(s1.at[g, st], r1.at[st, d - 1, idx], s1_s.at[st, d - 1, idx], s1_r.at[st, d - 1, idx], peer)

    def finish(r):
        gy, gx = tile_of(r)
        g = gy * SIDE + gx
        d0_copy(r, g).wait_recv()
        for st in range(2):
            put(s1.at[g, st], [own.at[g, c, st], r0.at[g, st]])

        @pl.when(lax.rem(r, SIDE) < SIDE - 1)
        def _():
            s1_copy(0, 1 + lax.rem(r, SIDE), g, gy, dev(z, y, gx, c)).start()

        @pl.when(r // SIDE < SIDE - 1)
        def _():
            s1_copy(1, 1 + r // SIDE, g, gx, dev(z, gy, x, c)).start()

    LAG = 3

    def step(r, carry):
        @pl.when(r < 16)
        def _():
            attend(r)

        @pl.when(r >= LAG)
        def _():
            finish(r - LAG)
        return carry

    lax.fori_loop(0, 8, step, 0)

    w_mate.wait_recv()
    for d in (1, 2, 3):
        zz = fwd(z, d)
        cp = rcopy(w1.at[:, pl.ds(pl.multiple_of(zz * 256, 256), 256)], wo_all.at[z, y, x, 1 - c],
                   wz_s.at[2 + d], wz_r.at[2 + d], z_peer[d])
        cp.start()
        wz.append(cp)
    wo_all[z, y, x, 1 - c] = w1[:, pl.ds(pl.multiple_of(z * 256, 256), 256)]

    lax.fori_loop(8, 16 + LAG, step, 0)

    for cp in wz:
        cp.wait_recv()
    wg1, wg2 = [], []
    for d in (1, 2, 3):
        for st, peer in ((0, x_peer[d]), (1, y_peer[d])):
            cp = rcopy(wo_all.at[:, y, x, st], wo_all.at[:, y, x, st], wg_s.at[0, st, d - 1], wg_r.at[0, st, d - 1], peer)
            cp.start()
            wg1.append(cp)

    s2c = []
    for d in (1, 2, 3, 0):
        for st in range(2):
            idx = fwd(y, d) if st == 0 else fwd(x, d)
            g = idx * SIDE + x if st == 0 else y * SIDE + idx
            for e in (1, 2, 3):
                s1_copy(st, e, g, idx, mate).wait_recv()
            put(s2.at[st, idx], [s1.at[g, st]] + [r1.at[st, e, idx] for e in range(3)])
            if d:
                cp = rcopy(s2.at[st, idx], r2.at[st, d - 1], s2_s.at[st, d - 1], s2_r.at[st, d - 1],
                           (y_peer if st == 0 else x_peer)[d])
                cp.start()
                s2c.append((st, d, cp))

    for cp in wg1:
        cp.wait_recv()
    for d in (1, 2, 3):
        for st, peer in ((0, y_peer[d]), (1, x_peer[d])):
            ref = wo_all.at[:, y, :, 0] if st == 0 else wo_all.at[:, :, x, 1]
            cp = rcopy(ref, ref, wg_s.at[1, st, d - 1], wg_r.at[1, st, d - 1], peer)
            cp.start()
            wg2.append(cp)

    s3c = []
    for st in range(2):
        for s, _, cp in s2c:
            if s == st:
                cp.wait_recv()
        put(s3.at[st], [s2.at[st, y if st == 0 else x]] + [r2.at[st, e] for e in range(3)])
        for d in (1, 2, 3):
            cp = rcopy(s3.at[st], r3.at[st, d - 1], s3_s.at[st, d - 1], s3_r.at[st, d - 1], z_peer[d])
            cp.start()
            s3c.append((st, cp))
    for st in range(2):
        for s, cp in s3c:
            if s == st:
                cp.wait_recv()
        data, _, total = combine([s3.at[st]] + [r3.at[st, e] for e in range(3)])
        for j in range(2):
            den = jnp.broadcast_to(total[:, 2 + j:3 + j], (8, 128))
            for k in range(2):
                osc[c, 2 * st + j, :, k * 128:(k + 1) * 128] = (data[2 * j + k] / den).astype(BF16)
    ocp = rcopy(osc.at[c], osc.at[c], o_s, o_r, mate)
    ocp.start()
    for cp in wg2:
        cp.wait_recv()
    ocp.wait_recv()

    acc = jnp.zeros((8, 256), F32)
    for h in range(8):
        wh = wo_all[h // 2, 2 * (h % 2):2 * (h % 2) + 2].reshape(256, 256)
        acc = acc + jnp.dot(osc[h // 4, h % 4], wh, preferred_element_type=F32)
    y_all[c, y, x, z] = acc.astype(BF16)

    yzc = []
    for d in (1, 2, 3):
        ref = y_all.at[c, y, x, z]
        cp = rcopy(ref, ref, yz_s.at[d - 1], yz_r.at[d - 1], z_peer[d])
        cp.start()
        yzc.append(cp)
    for cp in yzc:
        cp.wait_recv()
    yg, ydc = {}, []

    def half(st):
        return pl.ds(2 * st, 2)

    for d in (1, 2, 3):
        for st, peer in ((0, x_peer[d]), (1, y_peer[d])):
            ref = y_all.at[c, y, x, half(st)]
            cp = rcopy(ref, ref, yg_s.at[0, st, d - 1], yg_r.at[0, st, d - 1], peer)
            cp.start()
            yg[0, st, d] = cp
    for st in range(2):
        for d in (1, 2, 3):
            yg[0, st, d].wait_recv()
        ref = y_all.at[c, y, :, half(0)] if st == 0 else y_all.at[c, :, x, half(1)]
        for d in (1, 2, 3):
            cp = rcopy(ref, ref, yg_s.at[1, st, d - 1], yg_r.at[1, st, d - 1], (y_peer if st == 0 else x_peer)[d])
            cp.start()
            yg[1, st, d] = cp
        cp = rcopy(ref, ref, yd_s.at[st, 0], yd_r.at[st, 0], mate)
        cp.start()
        ydc.append(cp)
    for d in (1, 2, 3):
        for st in range(2):
            yg[1, st, d].wait_recv()
            if st == 0:
                ref = y_all.at[c, fwd(y, 4 - d), :, half(0)]
            else:
                ref = y_all.at[c, :, fwd(x, 4 - d), half(1)]
            cp = rcopy(ref, ref, yd_s.at[st, d], yd_r.at[st, d], mate)
            cp.start()
            ydc.append(cp)
    for cp in ydc:
        cp.wait_recv()
    out_ref[...] = y_all[...]

    def drain0(r, carry):
        gy, gx = tile_of(r)
        d0_copy(r, gy * SIDE + gx).wait_send()
        return carry

    lax.fori_loop(0, 16, drain0, 0)
    for d in (1, 2, 3):
        for idx in range(4):
            s1_copy(0, d, idx * SIDE + fwd(x, d), idx, mate).wait_send()
            s1_copy(1, d, fwd(y, d) * SIDE + idx, idx, mate).wait_send()
    for cp in [w_mate] + wz + wg1 + wg2 + [t[2] for t in s2c] + [t[1] for t in s3c] + [ocp] + yzc + list(yg.values()) + ydc:
        cp.wait_send()


def solution(mesh):
    def local_step(tokens, w_query, w_key, w_value, w_out, k_cache, v_cache, positions):
        n_rows, seq_local, head_dim = k_cache.shape
        shard_idx = lax.axis_index('sp')
        queries = jnp.dot(tokens, w_query, preferred_element_type=F32).astype(BF16)
        key_new = jnp.dot(tokens, w_key, preferred_element_type=F32).astype(BF16)
        value_new = jnp.dot(tokens, w_value, preferred_element_type=F32).astype(BF16)
        local_pos = positions - shard_idx * seq_local
        hit_mask = (jnp.arange(seq_local)[None, :] == local_pos[:, None])[:, :, None]
        k_upd = jnp.where(hit_mask, key_new[:, None, :], k_cache)
        v_upd = jnp.where(hit_mask, value_new[:, None, :], v_cache)
        vm = pl.BlockSpec(memory_space=pltpu.VMEM)
        msg = (5, 8, 128)
        dma = pltpu.SemaphoreType.DMA
        blocks = pl.pallas_call(
            attention_kernel,
            out_shape=jax.ShapeDtypeStruct((2, 4, 4, 4, 8, 256), BF16),
            in_specs=[pl.BlockSpec(memory_space=pltpu.SMEM), vm, vm, vm, vm],
            out_specs=vm,
            scratch_shapes=[
                pltpu.VMEM((16, 8, 8, 256), F32),
                pltpu.VMEM((16, 2, 2) + msg, F32),
                pltpu.VMEM((16, 2) + msg, F32),
                pltpu.VMEM((16, 2) + msg, F32),
                pltpu.VMEM((2, 3, 4) + msg, F32),
                pltpu.VMEM((2, 4) + msg, F32),
                pltpu.VMEM((2, 3) + msg, F32),
                pltpu.VMEM((2,) + msg, F32),
                pltpu.VMEM((2, 3) + msg, F32),
                pltpu.VMEM((2, 4, 8, 256), BF16),
                pltpu.VMEM((16, 1024), BF16),
                pltpu.VMEM((4, 4, 4, 2, 16, 256), BF16),
                pltpu.VMEM((2, 4, 4, 4, 8, 256), BF16),
                dma((16,)), dma((16,)), dma((7,)), dma((7,)), dma((2, 2, 3)), dma((2, 2, 3)),
                dma((2, 3, 4)), dma((2, 3, 4)), dma((2, 3)), dma((2, 3)), dma((2, 3)), dma((2, 3)),
                dma, dma, dma((3,)), dma((3,)), dma((2, 2, 3)), dma((2, 2, 3)), dma((2, 4)), dma((2, 4)),
            ],
            compiler_params=pltpu.CompilerParams(collective_id=0, has_side_effects=True,
                                                 vmem_limit_bytes=40 * 1024 * 1024),
        )(positions, queries, k_upd, v_upd, w_out)
        attn_out = blocks.transpose(1, 2, 4, 0, 3, 5).reshape(n_rows, 2048)
        return attn_out, k_upd, v_upd

    cache_spec = P('dp', 'sp', None)
    return jax.shard_map(local_step, mesh=mesh, in_specs=(P('dp', None), P(), P(), P(), P('sp', None), cache_spec, cache_spec, P('dp')), out_specs=(P('dp', None), cache_spec, cache_spec), check_vma=False)
```
